128 devices in a mesh: ctx: 16 (over y_hi, z, core), head: 8 (over y_lo, x).
Axes of the slice: x: 4, y: 4 (y_hi: 2, y_lo: 2; y = y_hi * 2 + y_lo), z: 4, core: 2. Of those that a mesh axis runs over, the one named last changes fastest.
Arguments:
- queries: bfloat16 [1024, 16384], P('ctx', 'head'), may hold values from -8000 to 8000
- key_codes: bfloat16 [32768, 1024], P('ctx', 'head'), may hold values from -127 to 127
- value_codes: bfloat16 [32768, 1024], P('ctx', 'head'), may hold values from -127 to 127
- key_scales: int32 [512, 8], P('ctx', 'head'), may hold values from 1 to 16
- value_scales: int32 [512, 8], P('ctx', 'head'), may hold values from 1 to 16
- positions: int32 [1024], replicated, may hold values from 0 to 32767
- out_weight: bfloat16 [16384, 16384], P('head', 'ctx'), may hold values from -0.046875 to 0.046875
Outputs:
- projected: bfloat16 [1024, 16384], P('head', 'ctx')
The draws below stay inside these ranges and needn't reach their ends.
All inputs are finite; a program needn't handle non-finite values.
Results may differ from the reference program's by a relative error of at most 0.009.
Values may be sent and summed in bfloat16 or wider, within the bound.
No kernel may reach another device: no remote copies, remote signals or barrier semaphores. Data moves between devices by JAX's collectives and lax.ppermute only.
A program may use at most 64 MiB of HBM per device.

```python
import math
import jax
import jax.numpy as jnp
from jax import lax

D = 16384
QH = 128
KVH = 8
HD = 128
BLOCK = 64
CTX = 32768
QROWS = 1024


def shared_codes(key):
    return jax.random.randint(jax.random.fold_in(key, 11), (CTX, KVH * HD), -127, 128)


def shared_positions(key):
    return jax.random.randint(jax.random.fold_in(key, 12), (QROWS,), 0, CTX)


def draw_key_codes(key, part):
    return shared_codes(key).astype(jnp.float32).astype(jnp.bfloat16)


def draw_value_codes(key, part):
    code_table = jax.random.randint(jax.random.fold_in(key, 13), (CTX, KVH * HD), -127, 128)
    return code_table.astype(jnp.float32).astype(jnp.bfloat16)


def draw_positions(key, part):
    return shared_positions(key)


def draw_queries(key, part):
    gaussian = jax.random.normal(jax.random.fold_in(key, 14), (QROWS, QH * HD), jnp.float32)
    return gaussian.astype(jnp.bfloat16)


def set_ends(entries, stream_key, least, top_value):
    dims = entries.shape
    place = [jax.random.randint(jax.random.fold_in(stream_key, axis), (), 0, dims[axis]) for axis in range(len(dims))]
    entries = entries.at[tuple(place)].set(least)
    longest = dims.index(max(dims))
    place[longest] = (place[longest] + 1) % dims[longest]
    return entries.at[tuple(place)].set(top_value)


def block_scale(own_key, extent, split, least, top_value):
    gain = 1.0
    for dim, shards_of in split:
        heights = jax.random.uniform(jax.random.fold_in(jax.random.fold_in(own_key, 6), dim), (shards_of,), jnp.float32, least / len(split), top_value / len(split))
        gain = gain * jnp.repeat(jnp.exp(heights), extent[dim] // shards_of).reshape((-1,) + (1,) * (len(extent) - 1 - dim))
    return gain


def bell_draw(rng, shape, spread, most, cuts=(), kind=jnp.bfloat16):
    result = spread * jax.random.normal(rng, shape, jnp.float32)
    if cuts:
        result = result * block_scale(rng, shape, cuts, -0.22, 0.18)
    return jnp.clip(result, -most, most).astype(kind)


def setup_inputs(seed: int = 0) -> dict:
    arg_keys = jax.random.split(jax.random.key(seed), 8)
    return {
        "queries": draw_queries(jax.random.fold_in(arg_keys[7], 71), 0),
        "key_codes": draw_key_codes(jax.random.fold_in(arg_keys[7], 71), 0),
        "value_codes": draw_value_codes(jax.random.fold_in(arg_keys[7], 71), 0),
        "key_scales": set_ends(jax.random.randint(arg_keys[3], (CTX // BLOCK, KVH), 1, 17), jax.random.fold_in(arg_keys[3], 1), 1, 16).astype(jnp.int32),
        "value_scales": set_ends(jax.random.randint(arg_keys[4], (CTX // BLOCK, KVH), 1, 17), jax.random.fold_in(arg_keys[4], 1), 1, 16).astype(jnp.int32),
        "positions": draw_positions(jax.random.fold_in(arg_keys[7], 71), 0),
        "out_weight": bell_draw(arg_keys[6], (QH * HD, D), (QH * HD) ** -0.5, 0.046875, ((0, 8), (1, 16))),
    }


QUANT_STEP = 1.0 / 2048.0
MASKED = -1e+30

def hadamard_signs(size_value):
    indices = jnp.arange(size_value, dtype=jnp.int32)
    common = jnp.bitwise_and(indices[:, None], indices[None, :])
    parity = jnp.zeros((size_value, size_value), jnp.int32)
    for shift_bit in range(max(int(size_value).bit_length(), 1)):
        parity = jnp.bitwise_xor(parity, jnp.bitwise_and(jnp.right_shift(common, shift_bit), 1))
    return 1.0 - 2.0 * parity.astype(jnp.float32)

def reference(queries, key_codes, value_codes, key_scales, value_scales, positions, out_weight):
    signs = hadamard_signs(HD)
    group_size = QH // KVH
    query_heads = queries.reshape(QROWS, QH, HD).astype(jnp.float32)
    rotated = jnp.einsum('rhd,de->rhe', query_heads, signs, precision=lax.Precision.HIGHEST) / math.sqrt(HD)
    key_factor = jnp.repeat(key_scales.astype(jnp.float32), BLOCK, axis=0) * (QUANT_STEP / math.sqrt(HD))
    value_factor = jnp.repeat(value_scales.astype(jnp.float32), BLOCK, axis=0) * QUANT_STEP
    key_pos = jnp.arange(CTX, dtype=jnp.int32)
    visible = key_pos[None, :] <= positions[:, None]

    def one_head(head_index):
        kv_index = head_index // group_size
        query_rows = lax.dynamic_index_in_dim(rotated, head_index, 1, keepdims=False)
        key_block = lax.dynamic_slice_in_dim(key_codes, (kv_index * HD).astype(jnp.int32), HD, 1).astype(jnp.float32)
        value_block = lax.dynamic_slice_in_dim(value_codes, (kv_index * HD).astype(jnp.int32), HD, 1)
        key_scale = lax.dynamic_index_in_dim(key_factor, kv_index, 1, keepdims=False)
        value_scale = lax.dynamic_index_in_dim(value_factor, kv_index, 1, keepdims=False)
        scores = jnp.dot(query_rows, key_block.T, preferred_element_type=jnp.float32, precision=lax.Precision.HIGHEST) * key_scale[None, :]
        scores = jnp.where(visible, scores, MASKED)
        highest = lax.optimization_barrier(jnp.max(scores, axis=1, keepdims=True))
        probs = jnp.where(visible, jnp.exp(scores - highest), 0.0)
        row_total = lax.optimization_barrier(jnp.sum(probs, axis=1, keepdims=True))
        weights = (probs * value_scale[None, :]).astype(jnp.bfloat16)
        numerator = jnp.dot(weights, value_block, preferred_element_type=jnp.float32)
        return (numerator / row_total).astype(jnp.bfloat16)
    normalized = lax.map(one_head, jnp.arange(QH, dtype=jnp.int32))
    attention = (jnp.einsum('hrd,de->hre', normalized.astype(jnp.float32), signs) / math.sqrt(HD)).astype(jnp.bfloat16)
    attention = jnp.transpose(attention, (1, 0, 2)).reshape(QROWS, QH * HD)
    return jnp.dot(attention, out_weight, preferred_element_type=jnp.float32).astype(jnp.bfloat16)
```

```python
import functools
import math

import jax
import jax.numpy as jnp
from jax import lax
from jax.experimental import pallas as pl
from jax.experimental.pallas import tpu as pltpu
from jax.sharding import PartitionSpec as P

HD = 128
BLOCK = 64
HEADS = 16
ROWS = 64
KEYS = 2048
CH = 512
LANES = 512
TILES = 4 * ROWS * HEADS // LANES
AUG = 16
QUANT_STEP = 1.0 / 2048.0
FLOOR = -1e30
HIDDEN = -3e38
SCALE = QUANT_STEP / HD * math.log2(math.e)
F32, BF16 = jnp.float32, jnp.bfloat16


def hadamard_signs(size_value):
    indices = jnp.arange(size_value, dtype=jnp.int32)
    common = jnp.bitwise_and(indices[:, None], indices[None, :])
    parity = jnp.zeros((size_value, size_value), jnp.int32)
    for shift_bit in range(max(int(size_value).bit_length(), 1)):
        parity = jnp.bitwise_xor(parity, jnp.bitwise_and(jnp.right_shift(common, shift_bit), 1))
    return 1.0 - 2.0 * parity.astype(jnp.float32)


def moved(value, dy=0, dz=0, dc=0):
    pairs = []
    for c in range(16):
        y, z, core = c >> 3, (c >> 1) & 3, c & 1
        source = (y ^ dy) * 8 + ((z + dz) % 4) * 2 + (core ^ dc)
        pairs.append((source, c))
    return lax.ppermute(value, "ctx", pairs)


def vmem(count):
    return [pl.BlockSpec(memory_space=pltpu.VMEM)] * count


def rows_to_lanes_kernel(perm_ref, q_ref, out_ref):
    rows = jnp.dot(perm_ref[...], q_ref[...], preferred_element_type=F32)
    for g in range(ROWS // 16):
        pieces = [rows[16 * g : 16 * g + 16, HD * h : HD * h + HD] for h in range(HEADS)]
        block = jnp.concatenate(pieces, axis=0)
        out_ref[:, 256 * g : 256 * g + 256] = block.T.astype(BF16)


def rows_to_lanes(perm, queries):
    return pl.pallas_call(
        rows_to_lanes_kernel,
        out_shape=jax.ShapeDtypeStruct((HD, ROWS * HEADS), BF16),
        in_specs=vmem(2),
        out_specs=vmem(1)[0],
        cost_estimate=pl.CostEstimate(flops=10**9, bytes_accessed=2**19, transcendentals=0),
        name="rows_to_lanes",
    )(perm, queries)


def attend_kernel(
    scalars, signs_ref, pos_ref, q0, q1, q2, q3, kv0, kv1, kv2, kv3, o0, o1, o2, o3,
    kaug, vaug, kscale, vscale, qtile, otile, qaug, s_a, s_b, top_a, top_b, top, acc,
):
    chunks = KEYS // CH
    per = CH // BLOCK
    lane = lax.broadcasted_iota(jnp.int32, (1, HD), 1)
    row16 = lax.broadcasted_iota(jnp.int32, (AUG, LANES), 0)
    signs = signs_ref[...]
    for j, kv in enumerate((kv0, kv1, kv2, kv3)):
        kscale[32 * j : 32 * j + 32] = kv[2 * KEYS : 2 * KEYS + 32].astype(F32) * SCALE
        vscale[32 * j : 32 * j + 32] = kv[2 * KEYS + 32 : 2 * KEYS + 64].astype(F32)

        def prepare(r, carry, j=j, kv=kv):
            first = pl.multiple_of(r * CH, CH)
            turned = jnp.dot(kv[pl.ds(first, CH), :], signs, preferred_element_type=F32)
            at = pl.multiple_of((j * chunks + r) * per, per)
            factors = kscale[pl.ds(at, per), :]
            inverse = 1.0 / vscale[pl.ds(at, per), :]
            target = j * chunks + r
            for b in range(per):
                exact = turned[BLOCK * b : BLOCK * b + BLOCK] * factors[b : b + 1]
                high = exact.astype(BF16)
                kaug[target, BLOCK * b : BLOCK * b + BLOCK, 0:HD] = high
                kaug[target, BLOCK * b : BLOCK * b + BLOCK, HD : 2 * HD] = (
                    exact - high.astype(F32)
                ).astype(BF16)
            values = kv[pl.ds(pl.multiple_of(KEYS + r * CH, CH), CH), :].astype(F32)
            vaug[target, 0:HD, :] = values.T.astype(BF16)
            shares = jnp.concatenate(
                [
                    jnp.where(lane < BLOCK, inverse[2 * i : 2 * i + 1], inverse[2 * i + 1 : 2 * i + 2])
                    for i in range(per // 2)
                ],
                axis=1,
            )
            high = shares.astype(BF16).astype(F32)
            low = shares - high
            extra = jnp.where(row16[:, :CH] == 0, high, jnp.where(row16[:, :CH] == 1, low, 0.0))
            vaug[target, HD : HD + AUG, :] = extra.astype(BF16)
            return carry

        lax.fori_loop(0, chunks, prepare, 0)
    for g in range(4):
        for pair, refs in enumerate(((q0, q1), (q2, q3))):
            for side, q in enumerate(refs):
                qtile[2 * g + pair, :, 256 * side : 256 * side + 256] = q[:, 256 * g : 256 * g + 256]

    def tile(t, carry):
        block = qtile[t]
        qaug[0:HD, :] = block
        qaug[HD : 2 * HD, :] = block
        pos = pos_ref[t]
        furthest = scalars[4 + t]
        base = [scalars[j] for j in range(4)]
        counts = [
            jnp.minimum(jnp.maximum(furthest - base[j] + CH, 0) // CH, chunks) for j in range(4)
        ]
        ends = [counts[0]]
        for j in range(1, 4):
            ends.append(ends[-1] + counts[j])
        total = ends[3]

        def place(i):
            index, first = i, base[0] + i * CH
            for j in range(1, 4):
                past = i >= ends[j - 1]
                step = i - ends[j - 1]
                index = jnp.where(past, j * chunks + step, index)
                first = jnp.where(past, base[j] + step * CH, first)
            beyond = i >= total
            return jnp.where(beyond, 0, index), jnp.where(beyond, 2**30, first)

        def produce(i, s_ref, top_ref):
            index, first = place(i)
            scores = jnp.dot(kaug[index], qaug[...], preferred_element_type=F32)
            key = lax.broadcasted_iota(jnp.int32, (CH, LANES), 0)
            scores = jnp.where(key <= pos - first, scores, HIDDEN)
            s_ref[...] = scores
            top_ref[...] = jnp.max(scores, axis=0, keepdims=True)

        def consume(i, s_ref, top_ref):
            index, _ = place(i)
            old = top[...]
            new = jnp.maximum(old, top_ref[...])
            fade = jnp.exp2(old - new)
            logs = jnp.log2(vscale[pl.ds(pl.multiple_of(index * per, per), per), :])
            weights = []
            for b in range(per):
                row = logs[b : b + 1]
                shift = new - jnp.concatenate([row] * (LANES // HD), axis=1)
                weights.append(
                    jnp.exp2(s_ref[BLOCK * b : BLOCK * b + BLOCK] - shift).astype(BF16)
                )
            weights = jnp.concatenate(weights, axis=0)
            acc[...] = acc[...] * fade + jnp.dot(
                vaug[index], weights, preferred_element_type=F32
            )
            top[...] = new

        top[...] = jnp.full_like(top, FLOOR)
        acc[...] = jnp.zeros_like(acc)
        produce(0, s_a, top_a)

        def step(n, carry):
            produce(2 * n + 1, s_b, top_b)
            consume(2 * n, s_a, top_a)
            produce(2 * n + 2, s_a, top_a)
            consume(2 * n + 1, s_b, top_b)
            return carry

        lax.fori_loop(0, (total + 1) // 2, step, 0)
        sums = acc[HD : HD + 1] + acc[HD + 1 : HD + 2]
        some = sums > 0.0
        inverse = jnp.where(some, 1.0 / jnp.where(some, sums, 1.0), 0.0)
        otile[t, 0:HD, :] = (acc[0:HD] * inverse).astype(BF16)
        lse = jnp.where(some, top[...] + jnp.log2(jnp.where(some, sums, 1.0)), FLOOR)
        high = lse.astype(BF16).astype(F32)
        rest = lse - high
        middle = rest.astype(BF16).astype(F32)
        low = rest - middle
        pieces = jnp.where(
            row16 == 0, high, jnp.where(row16 == 1, middle, jnp.where(row16 == 2, low, 0.0))
        )
        otile[t, HD : HD + AUG, :] = pieces.astype(BF16)
        return carry

    lax.fori_loop(0, TILES, tile, 0)
    for g in range(4):
        for pair, refs in enumerate(((o0, o1), (o2, o3))):
            for side, o in enumerate(refs):
                o[:, 256 * g : 256 * g + 256] = otile[2 * g + pair, :, 256 * side : 256 * side + 256]


def attend(scalars, signs, pos, queries, caches):
    chunks = 4 * KEYS // CH
    out = jax.ShapeDtypeStruct((HD + AUG, ROWS * HEADS), BF16)
    return pl.pallas_call(
        attend_kernel,
        out_shape=[out] * 4,
        in_specs=[pl.BlockSpec(memory_space=pltpu.SMEM)] + vmem(10),
        out_specs=vmem(4),
        scratch_shapes=[
            pltpu.VMEM((chunks, CH, 2 * HD), BF16),
            pltpu.VMEM((chunks, HD + AUG, CH), BF16),
            pltpu.VMEM((4 * KEYS // BLOCK, HD), F32),
            pltpu.VMEM((4 * KEYS // BLOCK, HD), F32),
            pltpu.VMEM((TILES, HD, LANES), BF16),
            pltpu.VMEM((TILES, HD + AUG, LANES), BF16),
            pltpu.VMEM((2 * HD, LANES), BF16),
            pltpu.VMEM((CH, LANES), F32),
            pltpu.VMEM((CH, LANES), F32),
            pltpu.VMEM((1, LANES), F32),
            pltpu.VMEM((1, LANES), F32),
            pltpu.VMEM((1, LANES), F32),
            pltpu.VMEM((HD + AUG, LANES), F32),
        ],
        cost_estimate=pl.CostEstimate(flops=3 * 10**10, bytes_accessed=2**23, transcendentals=2**25),
        compiler_params=pltpu.CompilerParams(vmem_limit_bytes=48 * 2**20),
        name="attend",
    )(scalars, signs, pos, *queries, *caches)


def merge_kernel(perm_ref, signs_ref, o0, o1, o2, o3, out_ref):
    parts = (o0, o1, o2, o3)
    lses = [jnp.sum(o[HD : HD + AUG].astype(F32), axis=0, keepdims=True) for o in parts]
    top = functools.reduce(jnp.maximum, lses)
    shares = [jnp.exp2(lse - top) for lse in lses]
    total = functools.reduce(jnp.add, shares)
    numerator = functools.reduce(
        jnp.add, [o[0:HD].astype(F32) * (share * QUANT_STEP) for o, share in zip(parts, shares)]
    )
    normalized = (numerator / total).astype(BF16)
    restored = jnp.dot(signs_ref[...], normalized, preferred_element_type=F32) * (
        1.0 / math.sqrt(HD)
    )
    columns = []
    turned = [restored[:, 256 * g : 256 * g + 256].T for g in range(4)]
    for h in range(HEADS):
        columns.append(
            jnp.concatenate([turned[g][16 * h : 16 * h + 16] for g in range(4)], axis=0)
        )
    rows = jnp.concatenate(columns, axis=1).astype(BF16)
    out_ref[...] = jnp.dot(perm_ref[...], rows, preferred_element_type=F32).astype(BF16)


def merge(perm, signs, parts):
    return pl.pallas_call(
        merge_kernel,
        out_shape=jax.ShapeDtypeStruct((ROWS, HEADS * HD), BF16),
        in_specs=vmem(6),
        out_specs=vmem(1)[0],
        cost_estimate=pl.CostEstimate(flops=10**9, bytes_accessed=2**20, transcendentals=0),
        name="merge",
    )(perm, signs, *parts)


def project_kernel(scalars, own_ref, other_ref, weight_ref, out_ref):
    d = pl.program_id(0)
    core = scalars[8]
    for side, ref in enumerate((own_ref, other_ref)):
        at = pl.multiple_of(jnp.where(core == side, 0, ROWS), ROWS)
        part = jnp.dot(ref[0], weight_ref[...], preferred_element_type=F32).astype(BF16)
        for e in range(2):
            out_ref[scalars[2 * d + e], pl.ds(at, ROWS), :] = part[ROWS * e : ROWS * e + ROWS]


def project(scalars, own, other, weight):
    width = weight.shape[1]
    return pl.pallas_call(
        project_kernel,
        out_shape=jax.ShapeDtypeStruct((8, 2 * ROWS, width), BF16),
        grid_spec=pltpu.PrefetchScalarGridSpec(
            num_scalar_prefetch=1,
            grid=(4,),
            in_specs=[
                pl.BlockSpec((1, 2 * ROWS, HEADS * HD), lambda d, s: (d, 0, 0)),
                pl.BlockSpec((1, 2 * ROWS, HEADS * HD), lambda d, s: (d, 0, 0)),
                pl.BlockSpec((HEADS * HD, width), lambda d, s: (0, 0)),
            ],
            out_specs=pl.BlockSpec((8, 2 * ROWS, width), lambda d, s: (0, 0, 0)),
        ),
        cost_estimate=pl.CostEstimate(flops=4 * 10**9, bytes_accessed=2**23, transcendentals=0),
        compiler_params=pltpu.CompilerParams(vmem_limit_bytes=48 * 2**20),
        name="project",
    )(scalars, own, other, weight)


def on_device(queries, key_codes, value_codes, key_scales, value_scales, positions, out_weight):
    place = lax.axis_index("ctx")
    y, z, core = place // 8, (place // 2) % 4, place % 2
    wide = (KEYS // BLOCK, HD)
    cache = jnp.concatenate(
        [
            key_codes,
            value_codes,
            jnp.broadcast_to(key_scales.astype(BF16), wide),
            jnp.broadcast_to(value_scales.astype(BF16), wide),
        ],
        axis=0,
    )
    cache_y = moved(cache, dy=1)
    cache_c = moved(cache, dc=1)
    cache_yc = moved(cache_y, dc=1)

    mine = lax.dynamic_slice(positions.reshape(2, 4, 2, ROWS), (y, 0, core, 0), (1, 4, 1, ROWS))
    mine = mine.reshape(4, ROWS)
    mine = lax.dynamic_slice(jnp.concatenate([mine, mine], axis=0), (z, 0), (4, ROWS))
    order = jnp.arange(ROWS, dtype=jnp.int32)
    before = (mine[:, None, :] < mine[:, :, None]) | (
        (mine[:, None, :] == mine[:, :, None]) & (order[None, :] < order[:, None])
    )
    rank = jnp.sum(before.astype(jnp.int32), axis=2)
    chosen = rank[:, :, None] == order[None, None, :]
    ordered = jnp.sum(jnp.where(chosen, mine[:, :, None], 0), axis=1)
    perm = chosen[0].astype(BF16)
    groups = ordered.reshape(4, 4, 1, 16)
    lanes = jnp.broadcast_to(groups, (4, 4, HEADS, 16)).reshape(2, 2, 4, 256)
    pos = lanes.transpose(2, 0, 1, 3).reshape(TILES, 1, LANES)
    furthest = jnp.max(groups.reshape(2, 2, 4, 16), axis=(1, 3)).T.reshape(TILES)
    bases = jnp.stack([y * 8 + core, y * 8 + 1 - core, (1 - y) * 8 + core, (1 - y) * 8 + 1 - core])
    scalars = jnp.concatenate([(bases + 2 * z) * KEYS, furthest]).astype(jnp.int32)

    signs = hadamard_signs(HD).astype(BF16)
    q0 = rows_to_lanes(perm.T, queries)
    blocks = (q0, moved(q0, dz=1), moved(q0, dz=2), moved(q0, dz=3))
    parts = attend(scalars, signs, pos, blocks, (cache, cache_c, cache_y, cache_yc))
    arrived = [parts[0]] + [moved(parts[d], dz=4 - d) for d in (1, 2, 3)]
    attention = merge(perm, signs, arrived)

    both = jnp.concatenate([attention, moved(attention, dy=1)], axis=0)
    own = jnp.stack([both, moved(both, dz=1), moved(both, dz=2), moved(both, dz=3)])
    other = moved(own, dc=1)
    steps = jnp.arange(4, dtype=jnp.int32)
    slots = jnp.stack([y * 4 + (z + steps) % 4, (1 - y) * 4 + (z + steps) % 4], axis=1)
    where = jnp.concatenate([slots.reshape(8), core[None]]).astype(jnp.int32)
    partial = project(where, own, other, out_weight)
    shares = lax.all_to_all(partial, "head", 0, 0)
    return jnp.sum(shares.astype(F32), axis=0).astype(BF16)


def solution(mesh):
    in_specs = (
        P("ctx", "head"),
        P("ctx", "head"),
        P("ctx", "head"),
        P("ctx", "head"),
        P("ctx", "head"),
        P(),
        P("head", "ctx"),
    )
    out_specs = P("head", "ctx")
    return jax.shard_map(
        on_device, mesh=mesh, in_specs=in_specs, out_specs=out_specs, check_vma=False
    )
```
